32 devices in a mesh: node: 4 (over x, core), local: 8 (over z, y).
Axes of the slice: x: 2, y: 2, z: 4, core: 2. Of those that a mesh axis runs over, the one named last changes fastest.
Arguments:
- tokens: bfloat16 [2048, 7168], P(('node', 'local')), may hold values from -6 to 6
- routes: int32 [2048, 2], P(('node', 'local')), may hold values from 0 to 7, as said below
- scores: float32 [2048, 2], P(('node', 'local')), may hold values from 0.1 to 1
- gate_proj: bfloat16 [32, 7168, 512], P(('node', 'local')), may hold values from -0.0625 to 0.0625
- up_proj: bfloat16 [32, 7168, 512], P(('node', 'local')), may hold values from -0.0625 to 0.0625
- down_proj: bfloat16 [32, 512, 7168], P(('node', 'local')), may hold values from -0.125 to 0.125
Outputs:
- combined: bfloat16 [2048, 7168], P(('node', 'local'))
The draws below stay inside these ranges and needn't reach their ends.
Inputs may be any that keep to these rules, and one draw needn't show every extreme that they name: `routes`: each row names 2 different experts. The rows of one device name each expert at most 20 times, and in every draw one expert is named by exactly 20 rows of every device.
All inputs are finite; a program needn't handle non-finite values.
Results may differ from the reference program's by a relative error of at most 0.0085.
Values may be sent and summed in bfloat16 or wider, within the bound.
A program may use at most 192 MiB of HBM per device.

```python
import math
import jax
import jax.numpy as jnp
from jax import lax

D = 7168
FF = 2048
SHARDS = 4
TOP = 2
TOK_DEV = 64
FF_DEV = 512
EXPERTS = 8
MOST = 20
TOKENS = 2048


def draw_routes(key, part):
    blocks = TOKENS // TOK_DEV
    base_key = jax.random.fold_in(key, 11)
    key_hot, key_cycle, key_perm, key_order = jax.random.split(base_key, 4)
    hot_expert = jax.random.randint(key_hot, (), 0, EXPERTS)
    cycle_least = max(TOP, (TOK_DEV * TOP - MOST + MOST - 1) // MOST)
    cycle_length = jax.random.randint(key_cycle, (blocks,), cycle_least, EXPERTS)
    shuffles = jax.vmap(lambda one_key: jax.random.permutation(one_key, EXPERTS - 1))(jax.random.split(key_perm, blocks))
    others = shuffles + (shuffles >= hot_expert).astype(shuffles.dtype)
    token_ids = jnp.arange(TOK_DEV)[:, None]
    slot_ids = jnp.arange(TOP)[None, :]
    leading = token_ids < MOST
    other_pos = jnp.where(leading, token_ids * (TOP - 1) + slot_ids - 1, MOST * (TOP - 1) + (token_ids - MOST) * TOP + slot_ids)
    cycle_pos = jnp.mod(other_pos[None, :, :], cycle_length[:, None, None])
    chosen = jnp.take_along_axis(others, cycle_pos.reshape(blocks, -1), axis=1).reshape(blocks, TOK_DEV, TOP)
    chosen = jnp.where((leading & (slot_ids == 0))[None, :, :], hot_expert, chosen)
    token_order = jax.vmap(lambda one_key: jax.random.permutation(one_key, TOK_DEV))(jax.random.split(key_order, blocks))
    chosen = jnp.take_along_axis(chosen, token_order[:, :, None], axis=1)
    return chosen.reshape(TOKENS, TOP).astype(jnp.int32)


def shard_levels(stream_key, shape, shards, low, largest):
    factor_of, own = 1.0, jax.random.fold_in(stream_key, 6)
    for position, shards_of in shards:
        draws = jnp.exp(jax.random.uniform(jax.random.fold_in(own, position), (shards_of,), jnp.float32, low / len(shards), largest / len(shards)))
        factor_of = factor_of * jnp.repeat(draws, shape[position] // shards_of).reshape([-1 if axis == position else 1 for axis in range(len(shape))])
    return factor_of


def noise(stream_key, dims, spread, bound, pieces=(), kind=jnp.bfloat16):
    level = shard_levels(stream_key, dims, pieces, -0.22, 0.18) if pieces else 1.0
    entries = jax.random.normal(stream_key, dims, jnp.float32) * spread * level
    return jnp.minimum(jnp.maximum(entries, -bound), bound).astype(kind)


def setup_inputs(seed: int = 0) -> dict:
    splits = jax.random.split(jax.random.key(seed), 7)
    return {
        "tokens": noise(splits[0], (TOKENS, D), 1.0, 6.0, ((0, 32),)),
        "routes": draw_routes(jax.random.fold_in(splits[6], 71), 0),
        "scores": jnp.clip(jnp.exp(math.log(1.0) - 2.3025851 * jax.random.uniform(splits[2], (TOKENS, TOP), jnp.float32) ** shard_levels(splits[2], (TOKENS, TOP), ((0, 32),), -0.2, 0.2)), 0.1, 1.0),
        "gate_proj": noise(splits[3], (EXPERTS * SHARDS, D, FF_DEV), D ** -0.5, 0.0625, ((0, 32),)),
        "up_proj": noise(splits[4], (EXPERTS * SHARDS, D, FF_DEV), D ** -0.5, 0.0625, ((0, 32),)),
        "down_proj": noise(splits[5], (EXPERTS * SHARDS, FF_DEV, D), FF ** -0.5, 0.125, ((0, 32),)),
    }


SCALE = 2.827


def reference(tokens, routes, scores, gate_proj, up_proj, down_proj):
    pair_count = TOKENS * TOP
    weights = (SCALE * scores / jnp.sum(scores, axis=1, keepdims=True)).astype(jnp.bfloat16)
    flat_exp = routes.reshape(-1).astype(jnp.int32)
    sort_order = jnp.argsort(flat_exp, stable=True).astype(jnp.int32)
    labels = jnp.arange(EXPERTS, dtype=jnp.int32)
    counts = jnp.sum((flat_exp[:, None] == labels[None, :]).astype(jnp.int32), axis=0).astype(jnp.int32)
    padded = (((counts + 127) // 128) * 128).astype(jnp.int32)
    group_ends = jnp.cumsum(padded).astype(jnp.int32)
    group_starts = (group_ends - padded).astype(jnp.int32)
    sorted_starts = (jnp.cumsum(counts) - counts).astype(jnp.int32)
    sorted_exp = flat_exp[sort_order]
    rank_list = jnp.arange(pair_count, dtype=jnp.int32)
    target_pos = (group_starts[sorted_exp] + rank_list - sorted_starts[sorted_exp]).astype(jnp.int32)
    block_count = (pair_count + 127) // 128 + EXPERTS
    slot_table = jnp.full((block_count * 128,), pair_count, jnp.int32).at[target_pos].set(sort_order)
    block_first = jnp.arange(block_count, dtype=jnp.int32) * 128
    block_exp = jnp.minimum(jnp.sum((group_ends[None, :] <= block_first[:, None]).astype(jnp.int32), axis=1), EXPERTS - 1).astype(jnp.int32)
    pair_weight = jnp.concatenate([weights.reshape(-1).astype(jnp.float32), jnp.zeros((1,), jnp.float32)])
    padded_x = jnp.concatenate([tokens, jnp.zeros((1, D), jnp.bfloat16)], axis=0)

    def accumulate(running, block_num):
        row_index = lax.dynamic_slice_in_dim(slot_table, (block_num * 128).astype(jnp.int32), 128)
        token_index = (row_index // TOP).astype(jnp.int32)
        expert = block_exp[block_num]
        row_data = padded_x[token_index]
        row_weight = pair_weight[row_index]
        first_row = (expert * SHARDS).astype(jnp.int32)
        w_gate = lax.dynamic_slice_in_dim(gate_proj, first_row, SHARDS, 0).transpose(1, 0, 2).reshape(D, FF)
        w_up = lax.dynamic_slice_in_dim(up_proj, first_row, SHARDS, 0).transpose(1, 0, 2).reshape(D, FF)
        gate_act = jnp.dot(row_data, w_gate, preferred_element_type=jnp.float32)
        up_act = jnp.dot(row_data, w_up, preferred_element_type=jnp.float32)
        hidden = (jax.nn.silu(gate_act) * up_act).astype(jnp.bfloat16)
        w_down = lax.dynamic_slice_in_dim(down_proj, first_row, SHARDS, 0)
        summed = jnp.zeros((128, D), jnp.float32)
        for shard_num in range(SHARDS):
            partial_value = jnp.dot(hidden[:, shard_num * FF_DEV:(shard_num + 1) * FF_DEV], w_down[shard_num], preferred_element_type=jnp.float32).astype(jnp.bfloat16)
            summed = summed + partial_value.astype(jnp.float32)
        running = running.at[token_index].add(summed * row_weight[:, None])
        return running, None

    running = lax.scan(accumulate, jnp.zeros((TOKENS + 1, D), jnp.float32), jnp.arange(block_count, dtype=jnp.int32))[0]
    return running[:TOKENS].astype(jnp.bfloat16)
```

```python
import functools

import jax
import jax.numpy as jnp
from jax import lax
from jax.experimental import pallas as pl
from jax.experimental.pallas import tpu as pltpu
from jax.sharding import PartitionSpec as P

SHARDS = 4
SCALE = 2.827
FOLD = 4
MESH = pl.DeviceIdType.MESH


def place(groups):
    node = lax.axis_index("node")
    local = lax.axis_index("local")
    mine = node * groups + local // SHARDS
    block = local % SHARDS
    near = block + 1 - 2 * (block % 2)
    far = (block + 2) % SHARDS
    corner = (near + 2) % SHARDS

    def device(expert, which):
        return (expert // groups, (expert % groups) * SHARDS + which)

    return mine, block, near, far, corner, device


def greet(mine, block, near, far, device, experts):
    barrier = pltpu.get_barrier_semaphore()
    targets = [device((mine + r) % experts, block) for r in range(1, experts)]
    targets += [device(mine, near), device(mine, far)]
    for target in targets:
        pl.semaphore_signal(barrier, inc=1, device_id=target, device_id_type=MESH)
    pl.semaphore_wait(barrier, len(targets))


def over_far(r, every):
    return every > 0 and r % every == 0


def rounds(experts, groups):
    same = [r for r in range(experts) if r % groups == 0]
    return same + [r for r in range(experts) if r % groups]


DISPATCH_FAR = 4
COMBINE_FAR = 0
AHEAD = 4
LAG = 2


class Transfer:
    def __init__(self, src, dst, send, recv, slot, target):
        self.copies = [
            pltpu.make_async_remote_copy(
                src_ref=piece,
                dst_ref=landing,
                send_sem=send.at[slot + (k,)],
                recv_sem=recv.at[slot + (k,)],
                device_id=target,
                device_id_type=MESH,
            )
            for k, (piece, landing) in enumerate(zip(src, dst))
        ]

    def start(self):
        for copy in self.copies:
            copy.start()

    def wait_recv(self):
        for copy in self.copies:
            copy.wait_recv()

    def wait_send(self):
        for copy in self.copies:
            copy.wait_send()


def at(refs, *index):
    return [ref.at[index] for ref in refs]


def dispatch_kernel(experts, groups, pieces, *refs):
    bucket, out = refs[:pieces], refs[pieces : 2 * pieces]
    own_sem, a_send, a_recv, b_send, b_recv, c_send, c_recv = refs[2 * pieces :]
    mine, block, near, far, corner, device = place(groups)
    greet(mine, block, near, far, device, experts)

    order = rounds(experts, groups)
    spread, to_near, to_far, relay = {}, {}, {}, {}
    for r in reversed(order[1:]):
        peer = (mine + r) % experts
        spread[r] = Transfer(at(bucket, peer), at(out, block, mine), a_send, a_recv, (r,), device(peer, block))
        spread[r].start()
    own = [
        pltpu.make_async_copy(src, dst, own_sem.at[k])
        for k, (src, dst) in enumerate(zip(at(bucket, mine), at(out, block, mine)))
    ]
    for copy in own:
        copy.start()

    def forward(r):
        source = (mine + experts - r) % experts
        if over_far(r, DISPATCH_FAR):
            to_near[r].wait_recv()
            moved = at(out, near, source)
            relay[r] = Transfer(moved, moved, c_send, c_recv, (r,), device(mine, far))
        else:
            to_far[r].wait_recv()
            moved = at(out, far, source)
            relay[r] = Transfer(moved, moved, c_send, c_recv, (r,), device(mine, near))
        relay[r].start()

    for step, r in enumerate(order):
        source = (mine + experts - r) % experts
        dst = at(out, block, source)
        if r == 0:
            src = at(bucket, mine)
        else:
            spread[r].wait_recv()
            src = dst
        to_near[r] = Transfer(src, dst, b_send, b_recv, (0, r), device(mine, near))
        to_far[r] = Transfer(src, dst, b_send, b_recv, (1, r), device(mine, far))
        to_near[r].start()
        to_far[r].start()
        if step >= LAG:
            forward(order[step - LAG])
    for r in order[experts - LAG :]:
        forward(r)
    for r in order:
        if over_far(r, DISPATCH_FAR):
            to_far[r].wait_recv()
        else:
            to_near[r].wait_recv()
        relay[r].wait_recv()
    for r in order:
        if r:
            spread[r].wait_send()
        to_near[r].wait_send()
        to_far[r].wait_send()
        relay[r].wait_send()
    for copy in own:
        copy.wait()


def combine_kernel(experts, groups, pieces, *refs):
    part, ret, held, total, back = [refs[k * pieces : (k + 1) * pieces] for k in range(5)]
    a_send, a_recv, b_send, b_recv, c_send, c_recv = refs[5 * pieces :]
    mine, block, near, far, corner, device = place(groups)
    greet(mine, block, near, far, device, experts)

    def add(dst, *terms):
        for k in range(pieces):
            value = terms[0][k][...].astype(jnp.float32)
            for term in terms[1:]:
                value = value + term[k][...].astype(jnp.float32)
            dst[k][...] = value.astype(dst[k].dtype)

    order = rounds(experts, groups)[::-1]
    relay, to_near, to_far, home = {}, {}, {}, {}

    def open_round(r):
        source = (mine + experts - r) % experts
        target = far if over_far(r, COMBINE_FAR) else near
        relay[r] = Transfer(at(part, corner, source), at(held, 2, r), c_send, c_recv, (r,), device(mine, target))
        relay[r].start()
        if over_far(r, COMBINE_FAR):
            to_far[r] = Transfer(at(part, far, source), at(held, 1, r), b_send, b_recv, (1, r), device(mine, far))
            to_far[r].start()
        else:
            to_near[r] = Transfer(at(part, near, source), at(held, 0, r), b_send, b_recv, (0, r), device(mine, near))
            to_near[r].start()

    def send_home(r):
        source = (mine + experts - r) % experts
        to_near[r].wait_recv()
        to_far[r].wait_recv()
        terms = at(part, block, source), at(held, 0, r), at(held, 1, r)
        if r == 0:
            add(at(ret, mine), *terms)
        else:
            add(at(back, r), *terms)
            home[r] = Transfer(at(back, r), at(ret, mine), a_send, a_recv, (r,), device(source, block))
            home[r].start()

    for r in order[:AHEAD]:
        open_round(r)
    for step, r in enumerate(order):
        source = (mine + experts - r) % experts
        relay[r].wait_recv()
        if over_far(r, COMBINE_FAR):
            add(at(total, r), at(part, near, source), at(held, 2, r))
            to_near[r] = Transfer(at(total, r), at(held, 0, r), b_send, b_recv, (0, r), device(mine, near))
            to_near[r].start()
        else:
            add(at(total, r), at(part, far, source), at(held, 2, r))
            to_far[r] = Transfer(at(total, r), at(held, 1, r), b_send, b_recv, (1, r), device(mine, far))
            to_far[r].start()
        if step + AHEAD < experts:
            open_round(order[step + AHEAD])
        if step >= LAG:
            send_home(order[step - LAG])
    for r in order[experts - LAG :]:
        send_home(r)
    for r in order:
        if r:
            home[r].wait_recv()
            home[r].wait_send()
        relay[r].wait_send()
        to_near[r].wait_send()
        to_far[r].wait_send()


def sems(experts, pieces):
    dma = pltpu.SemaphoreType.DMA
    one, two = dma((experts, pieces)), dma((2, experts, pieces))
    return [one, one, two, two, one, one]


def dispatch(bucket, groups):
    experts, pieces = bucket[0].shape[0], len(bucket)
    return pl.pallas_call(
        functools.partial(dispatch_kernel, experts, groups, pieces),
        out_shape=[jax.ShapeDtypeStruct((SHARDS,) + piece.shape, piece.dtype) for piece in bucket],
        in_specs=[pl.BlockSpec(memory_space=pltpu.VMEM)] * pieces,
        out_specs=[pl.BlockSpec(memory_space=pl.ANY)] * pieces,
        scratch_shapes=[pltpu.SemaphoreType.DMA((pieces,))] + sems(experts, pieces),
        compiler_params=pltpu.CompilerParams(collective_id=0, has_side_effects=True),
        name="dispatch",
    )(*bucket)


def combine(part, groups):
    experts, pieces = part[0].shape[1], len(part)
    blocks = [(piece.shape[1:], piece.dtype) for piece in part]
    return pl.pallas_call(
        functools.partial(combine_kernel, experts, groups, pieces),
        out_shape=[jax.ShapeDtypeStruct(shape, kind) for shape, kind in blocks],
        in_specs=[pl.BlockSpec(memory_space=pltpu.VMEM)] * pieces,
        out_specs=[pl.BlockSpec(memory_space=pltpu.VMEM)] * pieces,
        scratch_shapes=[pltpu.VMEM((3,) + shape, kind) for shape, kind in blocks]
        + [pltpu.VMEM(shape, kind) for shape, kind in blocks] * 2
        + sems(experts, pieces),
        compiler_params=pltpu.CompilerParams(
            collective_id=1, has_side_effects=True, vmem_limit_bytes=60 * 2**20
        ),
        name="combine",
    )(*part)


def dot(left, right):
    return jnp.dot(left, right, preferred_element_type=jnp.float32)


def activate(gate_act, up_act):
    return (jax.nn.silu(gate_act) * up_act).astype(jnp.bfloat16)


def expert_block(rows, w_gate, w_up, w_down):
    hidden = activate(dot(rows, w_gate), dot(rows, w_up))
    return dot(hidden, w_down).astype(jnp.bfloat16)


def folded_block(rows, w_gate, w_up, w_down):
    half = rows.shape[1]

    def project(weight):
        left = dot(rows, weight[:half]).reshape(-1, 2, FOLD, weight.shape[1])
        right = dot(rows, weight[half:]).reshape(-1, 2, FOLD, weight.shape[1])
        return left[:, 0] + right[:, 1]

    hidden = activate(project(w_gate), project(w_up))
    twice = jnp.concatenate([hidden, hidden], axis=1).reshape(rows.shape[0], -1)
    upper = jnp.arange(rows.shape[0])[:, None] % (2 * FOLD) < FOLD
    return jnp.where(upper, dot(twice, w_down[:, :half]), dot(twice, w_down[:, half:])).astype(jnp.bfloat16)


def bucketed(tokens, routes, scores, gate_proj, up_proj, down_proj):
    node_count = lax.axis_size("node")
    local_count = lax.axis_size("local")
    token_count, model_width = tokens.shape
    top_count = routes.shape[1]
    groups = local_count // SHARDS
    experts = node_count * groups
    per_expert = max(
        2, token_count * top_count // experts + token_count * top_count // (4 * experts)
    )
    tile = 2 * FOLD
    half = model_width // 2
    full = per_expert // tile * tile
    folds = full > 0 and 0 < per_expert - full <= FOLD
    if not folds:
        full = (per_expert + tile - 1) // tile * tile
    cap = full + FOLD if folds else full
    weights = (SCALE * scores / jnp.sum(scores, axis=1, keepdims=True)).astype(jnp.bfloat16)
    labels = jnp.arange(experts, dtype=jnp.int32)
    matches = routes[:, :, None] == labels[None, None, :]
    routed = jnp.any(matches, axis=1)
    dense_weight = jnp.sum(jnp.where(matches, weights.astype(jnp.float32)[:, :, None], 0.0), axis=1)
    position = jnp.cumsum(routed.astype(jnp.int32), axis=0) - 1
    slot_ids = jnp.arange(cap, dtype=jnp.int32)
    pick = routed.T[:, None, :] & (position.T[:, None, :] == slot_ids[None, :, None])
    slot_pick = pick.astype(jnp.bfloat16)
    slot_weight = jnp.where(pick, dense_weight.T[:, None, :], 0.0).astype(jnp.bfloat16)

    def flat(slots):
        return slots.reshape(-1, slots.shape[-1])

    def halves(slots):
        none = jnp.zeros_like(slots)
        return flat(jnp.concatenate([slots, none], axis=1)), flat(jnp.concatenate([none, slots], axis=1))

    bucket = [dot(flat(slot_pick[:, :full]), tokens).astype(jnp.bfloat16).reshape(experts, full, model_width)]
    if folds:
        upper, lower = halves(slot_pick[:, full:])
        folded = (dot(upper, tokens[:, :half]) + dot(lower, tokens[:, half:])).astype(jnp.bfloat16)
        bucket.append(folded.reshape(experts, tile, half))
    gathered = dispatch(bucket, groups)
    blocks = expert_block, folded_block
    part = [
        blocks[k](flat(piece), gate_proj[0], up_proj[0], down_proj[0]).reshape(piece.shape)
        for k, piece in enumerate(gathered)
    ]
    returned = combine(part, groups)
    combined = dot(flat(slot_weight[:, :full]).T, flat(returned[0]))
    if folds:
        upper, lower = halves(slot_weight[:, full:])
        rows = flat(returned[1])
        combined = combined + jnp.concatenate([dot(upper.T, rows), dot(lower.T, rows)], axis=1)
    return combined.astype(jnp.bfloat16)


CORES = 2
SQUARES = 4
PARTS = 2
DISPATCH_VIA_FAR = (1, 5,)
COMBINE_VIA_FAR = (0,)
SCHEDULE = [
    ("spread", 5), ("spread", 3), ("spread", 1), ("far", 0), ("near", 0), ("near", 4),
    ("tables", 0), ("spread", 6), ("near", 5), ("near", 1), ("far", 3), ("swap1", 5),
    ("far", 6), ("near", 3), ("spread", 7), ("far", 1), ("swap0", 5), ("pass_on", 0),
    ("pass_on", 1), ("swap0", 6), ("pass_on", 3), ("share", 0), ("near", 6), ("far", 7),
    ("pass_on", 6), ("far", 4), ("share", 3), ("compute", 0), ("spread", 2), ("swap2", 6),
    ("near", 7), ("swap1", 6), ("compute", 3), ("share", 1), ("swap3", 6), ("swap0", 7),
    ("pass_on", 7), ("join", 3), ("hop", 3), ("join", 0), ("swap1", 4), ("swap0", 4),
    ("pass_on", 5), ("compute", 1), ("far", 5), ("share", 7), ("swap1", 7), ("swap3", 7),
    ("swap2", 4), ("hop", 0), ("join", 1), ("pass_on", 4), ("far", 2), ("near", 2),
    ("swap2", 7), ("hop", 1), ("compute", 7), ("swap3", 4), ("side", 3), ("middle", 3),
    ("share", 6), ("swap3", 5), ("swap2", 5), ("join", 7), ("compute", 6), ("share", 4),
    ("side", 0), ("pass_on", 2), ("share", 5), ("side", 1), ("join", 6), ("middle", 1),
    ("hop", 6), ("finish", 3), ("share", 2), ("compute", 4), ("hop", 7), ("compute", 2),
    ("middle", 6), ("join", 4), ("side", 6), ("join", 2), ("middle", 7), ("side", 7),
    ("compute", 5), ("finish", 6), ("hop", 2), ("join", 5), ("hop", 5), ("middle", 0),
    ("side", 2), ("middle", 2), ("finish", 7), ("hop", 4), ("middle", 5), ("finish", 2),
    ("finish", 1), ("side", 5), ("side", 4), ("middle", 4), ("finish", 0), ("finish", 5),
    ("finish", 4),
]


class Flow:
    def __init__(self, **spec):
        self.spec = spec
        self.started = self.sent = self.landed = False

    def start(self):
        self.copy = pltpu.make_async_remote_copy(device_id_type=MESH, **self.spec)
        self.copy.start()
        self.started = True

    def wait_send(self):
        if self.started and not self.sent:
            self.copy.wait_send()
        self.sent = True

    def wait_recv(self):
        if self.started and not self.landed:
            self.copy.wait_recv()
        self.landed = True


def slots_of(token_count, top_count, experts):
    per_expert = max(2, token_count * top_count // experts + token_count * top_count // (4 * experts))
    seen = CORES * per_expert
    return seen, token_count - seen, 2 * seen - token_count


def flip(value, by):
    return 1 - value if by else value


def prepare_kernel(groups, private, shared, table_ref, tokens_ref, lists_ref, pick_ref, weight_ref):
    node = lax.axis_index("node")
    local = lax.axis_index("local")
    side, core, half = node // CORES, node % CORES, local // SHARDS
    count = table_ref.shape[1]
    listed = count // 2
    swap = shared // 2
    first, second = table_ref[0:1, :], table_ref[1:2, :]
    score_first, score_second = table_ref[2:3, :], table_ref[3:4, :]
    total = score_first + score_second
    weight_first = (SCALE * score_first / total).astype(jnp.bfloat16).astype(jnp.float32)
    weight_second = (SCALE * score_second / total).astype(jnp.bfloat16).astype(jnp.float32)

    def named(expert):
        name = expert.astype(jnp.float32)
        return jnp.where(first == name, 1.0, 0.0) + jnp.where(second == name, 1.0, 0.0)

    def weight_row(expert):
        name = expert.astype(jnp.float32)
        return jnp.where(first == name, weight_first, 0.0) + jnp.where(second == name, weight_second, 0.0)

    def expert_at(dx, dh, dc):
        return (flip(side, dx) * CORES + flip(core, dc)) * groups + flip(half, dh)

    row = lax.broadcasted_iota(jnp.int32, (count, count), 0)
    col = lax.broadcasted_iota(jnp.int32, (count, count), 1)
    before = jnp.where(row < col, 1.0, 0.0).astype(jnp.bfloat16)
    slot = row.astype(jnp.float32)
    picks = []
    for dh in range(2):
        on = [jnp.minimum(named(expert_at(dx, dh, 0)) + named(expert_at(dx, dh, 1)), 1.0) for dx in range(2)]
        both = on[0] * on[1]
        only = [on[0] - both, on[1] - both]
        stack = jnp.concatenate([both, only[0], only[1], jnp.zeros((5, count), jnp.float32)], axis=0)
        rank = dot(stack.astype(jnp.bfloat16), before)
        both_rank = rank[0:1]
        both_count = jnp.sum(both, axis=1, keepdims=True)
        spilled = jnp.maximum(both_count - shared, 0.0)
        held = jnp.minimum(both_count, float(shared))

        def shared_slot(index):
            return jnp.where(index < swap, private + index, listed + private + index - swap)

        place = [spilled + rank[1:2], spilled + rank[2:3]]
        over = [shared_slot(held + place[0] - private), shared_slot(shared - 1 - (place[1] - private))]
        main = jnp.where(both_rank < shared, shared_slot(both_rank), both_rank - shared)
        main = jnp.where(both > 0, main, -1.0)
        for dx in range(2):
            here = jnp.where(place[dx] < private, dx * listed + place[dx], over[dx])
            main = jnp.where(only[dx] > 0, here, main)
        again = jnp.where((both > 0) & (both_rank >= shared), listed + both_rank - shared, -1.0)
        pick = jnp.where((slot == main) | (slot == again), 1.0, 0.0)
        picks.append(pick)
        for dx in range(2):
            mine = pick[dx * listed : (dx + 1) * listed]
            other = pick[(1 - dx) * listed + private : (2 - dx) * listed]
            r = 2 * dh + dx
            seen = jnp.concatenate(
                [mine, other, jnp.zeros((128 - listed - swap, count), jnp.float32)], axis=0
            ).astype(jnp.bfloat16)
            rows = jnp.concatenate(
                [weight_row(expert_at(dx, dh, dc)) for dc in range(2)] + [jnp.zeros((6, count), jnp.float32)], axis=0
            ).astype(jnp.bfloat16)
            values = lax.dot_general(rows, seen, (((1,), (1,)), ((), ())), preferred_element_type=jnp.float32)
            for dc in range(2):
                weight_ref[r, dc] = jnp.broadcast_to(values[dc : dc + 1], (8, 128))
    pick = jnp.concatenate(picks, axis=0).astype(jnp.bfloat16)
    pick_ref[...] = pick
    width = 1024

    def fill(step, carry):
        columns = pl.ds(pl.multiple_of(step * width, width), width)
        rows = dot(pick, tokens_ref[:, columns]).astype(jnp.bfloat16)
        for r in range(SQUARES):
            lists_ref[r, :, columns] = rows[r * listed : (r + 1) * listed]
        return carry

    lax.fori_loop(0, tokens_ref.shape[1] // width, fill, 0)


def prepare(table, tokens, groups, private, shared):
    count, model_width = tokens.shape
    vmem = pl.BlockSpec(memory_space=pltpu.VMEM)
    return pl.pallas_call(
        functools.partial(prepare_kernel, groups, private, shared),
        out_shape=[
            jax.ShapeDtypeStruct((SQUARES, count // 2, model_width), jnp.bfloat16),
            jax.ShapeDtypeStruct((2 * count, count), jnp.bfloat16),
            jax.ShapeDtypeStruct((SQUARES, CORES, 8, 128), jnp.float32),
        ],
        in_specs=[vmem, vmem],
        out_specs=[vmem] * 3,
        name="prepare",
    )(table, tokens)


def layer_kernel(
    listed, swap, lists, weight, gate_hbm, up_hbm, down_hbm, ret,
    gate, up, down, rows_a, rows_b, table, given_a, given_b, extra, held_a, held_b, hidden,
    load_sem, own_sem, t_send, t_recv, send, recv,
):
    node = lax.axis_index("node")
    local = lax.axis_index("local")
    side, core = node // CORES, node % CORES
    half, block = local // SHARDS, local % SHARDS
    deep, across = block // 2, block % 2
    part = listed // PARTS
    rows, given, held = (rows_a, rows_b), (given_a, given_b), (held_a, held_b)
    lane = [rows[p].shape[2] for p in range(PARTS)]

    def device(r, dc, db):
        to_block = flip(deep, db // 2) * 2 + flip(across, db % 2)
        return (flip(side, r % 2) * CORES + flip(core, dc), flip(half, r // 2) * SHARDS + to_block)

    offsets = [(r, dc, db) for r in range(SQUARES) for dc in range(CORES) for db in range(SHARDS)][1:]
    barrier = pltpu.get_barrier_semaphore()
    for offset in offsets:
        pl.semaphore_signal(barrier, inc=1, device_id=device(*offset), device_id_type=MESH)

    loads = [
        pltpu.make_async_copy(src.at[0], dst, load_sem.at[k])
        for k, (src, dst) in enumerate(((gate_hbm, gate), (up_hbm, up), (down_hbm, down)))
    ]
    own = [
        pltpu.make_async_copy(
            lists.at[0, pl.ds(p * part, part)], rows[p].at[0, 0, pl.ds(0, part)], own_sem.at[p]
        )
        for p in range(PARTS)
    ]
    own.append(pltpu.make_async_copy(weight.at[0, 0], table.at[0, 0, 0], own_sem.at[PARTS]))
    for copy in own + loads:
        copy.start()
    pl.semaphore_wait(barrier, len(offsets))
    waited = set()

    def once(*names):
        for name in names:
            if name not in waited:
                waited.add(name)
                (own + loads)[name].wait()

    everything = []

    def flow(kind, q, there, src, dst, target):
        made = Flow(
            src_ref=src, dst_ref=dst, send_sem=send.at[kind, q], recv_sem=recv.at[kind, there], device_id=target
        )
        everything.append(made)
        return made

    def piece(ref, r, p):
        return ref.at[r, pl.ds(p * part, part)]

    def entry(q, db):
        return rows[q // SQUARES].at[q % SQUARES, 0, pl.ds(db * part, part)]

    def last_rows(r, db):
        return rows[1].at[r, 0, pl.ds(db * part + part - swap, swap)]

    def other_rows(r, db):
        return rows[1].at[r, 0, pl.ds(SHARDS * part + db * swap, swap)]

    def other(q):
        return q + 1 - 2 * (q % 2)

    spread, near, far, relay, shared = {}, {}, {}, {}, {}
    out, hop, side_sum, far_sum, home, swapped, patch = {}, {}, {}, {}, {}, {}, {}
    y_way, z_way = device(0, 0, 1), device(0, 0, 2)
    for q in range(PARTS * SQUARES):
        p, r = q // SQUARES, q % SQUARES
        first = entry(q, 0) if r else piece(lists, 0, p)
        if r:
            spread[q] = flow(0, q, q, piece(lists, r, p), entry(q, 0), device(r, 0, 0))
            home[q] = flow(9, q, q, entry(q, 0), piece(ret, r, p), device(r, 0, 0))
        near[q] = flow(1, q, q, first, entry(q, 1), y_way)
        far[q] = flow(2, q, q, first, entry(q, 2), z_way)
        if q in DISPATCH_VIA_FAR:
            relay[q] = flow(3, q, q, entry(q, 1), entry(q, 3), z_way)
        else:
            relay[q] = flow(3, q, q, entry(q, 2), entry(q, 3), y_way)
        shared[q] = flow(4, q, q, rows[p].at[r, 0], rows[p].at[r, 1], device(0, 1, 0))
        out[q] = flow(5, q, q, rows[p].at[r, 1], given[p].at[r], device(0, 1, 0))
        early, late = (2, 1) if q in COMBINE_VIA_FAR else (1, 2)
        early_way, late_way = device(0, 0, early), device(0, 0, late)
        hop[q] = flow(6, q, q, entry(q, 3), held[p].at[2, r], early_way)
        side_sum[q] = flow(7, q, q, entry(q, early), held[p].at[0, r], early_way)
        far_sum[q] = flow(8, q, q, held[p].at[2, r], held[p].at[1, r], late_way)
        if p:
            for db in range(SHARDS):
                swapped[q, db] = flow(
                    10 + db, q, other(q), last_rows(r, db), other_rows(other(r), db), device(1, 0, 0)
                )
                patch[q, db] = flow(
                    14 + db,
                    q,
                    other(q),
                    other_rows(r, db),
                    extra.at[other(r), pl.ds(db * swap, swap)],
                    device(1, 0, 0),
                )
    tables = [
        Flow(
            src_ref=weight.at[r, dc],
            dst_ref=table.at[r, dc, db],
            send_sem=t_send.at[r, dc, db],
            recv_sem=t_recv.at[r, dc, db],
            device_id=device(r, dc, db),
        )
        for r, dc, db in offsets
    ]
    everything.extend(tables)

    def add_into(target, *terms):
        value = target[...].astype(jnp.float32)
        for term in terms:
            value = value + term[...].astype(jnp.float32)
        target[...] = value.astype(target.dtype)

    def landed(q, db):
        if db == 0:
            if q % SQUARES:
                spread[q].wait_recv()
            else:
                once(q // SQUARES)
        else:
            (None, near, far, relay)[db][q].wait_recv()

    def send_near(q):
        if q % SQUARES:
            spread[q].wait_recv()
        near[q].start()

    def send_far(q):
        if q % SQUARES:
            spread[q].wait_recv()
        far[q].start()

    def pass_on(q):
        landed(q, 1 if q in DISPATCH_VIA_FAR else 2)
        relay[q].start()

    def swap_rows(q, db):
        landed(q, db)
        swapped[q, db].start()

    def share(q):
        for db in range(SHARDS):
            landed(q, db)
        if q >= SQUARES:
            for db in range(SHARDS):
                swapped[other(q), db].wait_recv()
        shared[q].start()

    def column(q):
        p, r = q // SQUARES, q % SQUARES
        spans = [(part, p * part)] + ([(swap, listed)] if p else [])
        values = []
        for dc in range(CORES):
            for size, shift in spans:
                lanes = lax.broadcasted_iota(jnp.int32, (size, 128), 1)
                spots = lax.broadcasted_iota(jnp.int32, (size, 128), 0) + shift
                for db in range(SHARDS):
                    chosen = jnp.where(lanes == spots, table[r, dc, db, 0:1, :], 0.0)
                    values.append(jnp.sum(chosen, axis=1, keepdims=True))
        return jnp.concatenate(values, axis=0)

    def compute(q):
        p, r = q // SQUARES, q % SQUARES
        once(PARTS, PARTS + 1, PARTS + 2)
        for copy in tables:
            copy.wait_recv()
        shared[q].wait_recv()
        size = CORES * lane[p]
        scale = column(q)
        tile = 256

        def open_up(step, carry):
            columns = pl.ds(pl.multiple_of(step * tile, tile), tile)
            left = rows[p][r].reshape(size, down.shape[1])
            gate_act = dot(left, gate[:, columns])
            up_act = dot(left, up[:, columns])
            hidden[:size, columns] = (jax.nn.silu(gate_act) * up_act * scale).astype(jnp.bfloat16)
            return carry

        lax.fori_loop(0, gate.shape[1] // tile, open_up, 0)
        once(PARTS + 3)
        for sent in [near[q], far[q], relay[q], shared[q]] + [swapped[q, db] for db in range(SHARDS) if p]:
            sent.wait_send()
        wide = 1024

        def close(step, carry):
            columns = pl.ds(pl.multiple_of(step * wide, wide), wide)
            result = dot(hidden[:size], down[:, columns]).astype(jnp.bfloat16)
            rows[p][r, 0, :, columns] = result[: lane[p]]
            rows[p][r, 1, :, columns] = result[lane[p] :]
            return carry

        lax.fori_loop(0, down.shape[1] // wide, close, 0)
        out[q].start()

    def join(q):
        p, r = q // SQUARES, q % SQUARES
        out[q].wait_recv()
        if p:
            for db in (3, 1, 2, 0):
                add_into(other_rows(r, db), given[p].at[r, pl.ds(SHARDS * part + db * swap, swap)])
                patch[q, db].start()
        for db in range(SHARDS):
            add_into(entry(q, db), given[p].at[r, pl.ds(db * part, part)])

    def mended(q, db):
        if q >= SQUARES:
            patch[other(q), db].wait_recv()
            add_into(last_rows(q % SQUARES, db), extra.at[q % SQUARES, pl.ds(db * swap, swap)])

    def send_hop(q):
        mended(q, 3)
        hop[q].start()

    def send_side(q):
        mended(q, 2 if q in COMBINE_VIA_FAR else 1)
        side_sum[q].start()

    def middle(q):
        late = 1 if q in COMBINE_VIA_FAR else 2
        mended(q, late)
        hop[q].wait_recv()
        add_into(held[q // SQUARES].at[2, q % SQUARES], entry(q, late))
        far_sum[q].start()

    def finish(q):
        p, r = q // SQUARES, q % SQUARES
        mended(q, 0)
        side_sum[q].wait_recv()
        far_sum[q].wait_recv()
        if r:
            add_into(entry(q, 0), held[p].at[0, r], held[p].at[1, r])
            home[q].start()
        else:
            value = entry(q, 0)[...].astype(jnp.float32)
            value = value + held[p][0, r].astype(jnp.float32) + held[p][1, r].astype(jnp.float32)
            piece(ret, 0, p)[...] = value.astype(ret.dtype)

    steps = dict(
        spread=lambda q: spread[q].start(), near=send_near, far=send_far, pass_on=pass_on, share=share,
        compute=compute, join=join, hop=send_hop, side=send_side, middle=middle, finish=finish,
        tables=lambda q: [copy.start() for copy in tables],
    )
    for db in range(SHARDS):
        steps[f"swap{db}"] = functools.partial(swap_rows, db=db)
    for name, q in SCHEDULE:
        steps[name](q)
    once(*range(PARTS + 4))
    for made in everything:
        made.wait_recv()
        made.wait_send()


def layer(lists, weight, gate_proj, up_proj, down_proj, swap):
    _, listed, model_width = lists.shape
    hidden_width = gate_proj.shape[2]
    part = listed // PARTS
    lanes = (SHARDS * part, SHARDS * (part + swap))
    dma = pltpu.SemaphoreType.DMA
    vmem = pl.BlockSpec(memory_space=pltpu.VMEM)
    hbm = pl.BlockSpec(memory_space=pl.ANY)

    def space(*shape):
        return pltpu.VMEM(shape, jnp.bfloat16)

    return pl.pallas_call(
        functools.partial(layer_kernel, listed, swap),
        out_shape=jax.ShapeDtypeStruct(lists.shape, jnp.bfloat16),
        in_specs=[vmem, vmem, hbm, hbm, hbm],
        out_specs=vmem,
        scratch_shapes=[
            space(*gate_proj.shape[1:]),
            space(*up_proj.shape[1:]),
            space(*down_proj.shape[1:]),
            space(SQUARES, CORES, lanes[0], model_width),
            space(SQUARES, CORES, lanes[1], model_width),
            pltpu.VMEM((SQUARES, CORES, SHARDS, 8, 128), jnp.float32),
            space(SQUARES, lanes[0], model_width),
            space(SQUARES, lanes[1], model_width),
            space(SQUARES, SHARDS * swap, model_width),
            space(3, SQUARES, part, model_width),
            space(3, SQUARES, part, model_width),
            space(CORES * lanes[1], hidden_width),
            dma((3,)),
            dma((PARTS + 1,)),
            dma((SQUARES, CORES, SHARDS)),
            dma((SQUARES, CORES, SHARDS)),
            dma((18, PARTS * SQUARES)),
            dma((18, PARTS * SQUARES)),
        ],
        compiler_params=pltpu.CompilerParams(
            collective_id=2, has_side_effects=True, vmem_limit_bytes=67043328
        ),
        name="layer",
    )(lists, weight, gate_proj, up_proj, down_proj)


def per_device(tokens, routes, scores, gate_proj, up_proj, down_proj):
    node_count = lax.axis_size("node")
    local_count = lax.axis_size("local")
    token_count, top_count = routes.shape
    groups = local_count // SHARDS
    experts = node_count * groups
    seen, private, shared = slots_of(token_count, top_count, experts)
    square = node_count == 2 * CORES and groups == 2 and top_count == 2
    fits = private > 0 and shared > 0 and private % 8 == 0 and shared % 16 == 0 and token_count % 32 == 0
    if not (square and fits):
        return bucketed(tokens, routes, scores, gate_proj, up_proj, down_proj)
    table = jnp.concatenate([routes.astype(jnp.float32), scores], axis=1).T
    lists, pick, weight = prepare(table, tokens, groups, private, shared)
    returned = layer(lists, weight, gate_proj, up_proj, down_proj, shared // 2)
    flat = returned.reshape(-1, returned.shape[-1])
    combined = lax.dot_general(pick, flat, (((0,), (0,)), ((), ())), preferred_element_type=jnp.float32)
    return combined.astype(jnp.bfloat16)


def solution(mesh):
    return jax.shard_map(
        per_device,
        mesh=mesh,
        in_specs=(
            P(("node", "local"), None),
            P(("node", "local"), None),
            P(("node", "local"), None),
            P(("node", "local"), None, None),
            P(("node", "local"), None, None),
            P(("node", "local"), None, None),
        ),
        out_specs=P(("node", "local"), None),
        check_vma=False,
    )
```

```python
import functools

import jax
import jax.numpy as jnp
from jax import lax
from jax.experimental import pallas as pl
from jax.experimental.pallas import tpu as pltpu
from jax.sharding import PartitionSpec as P

SHARDS = 4
SCALE = 2.827
FOLD = 4
MESH = pl.DeviceIdType.MESH


def place(groups):
    node = lax.axis_index("node")
    local = lax.axis_index("local")
    mine = node * groups + local // SHARDS
    block = local % SHARDS
    near = block + 1 - 2 * (block % 2)
    far = (block + 2) % SHARDS
    corner = (near + 2) % SHARDS

    def device(expert, which):
        return (expert // groups, (expert % groups) * SHARDS + which)

    return mine, block, near, far, corner, device


def greet(mine, block, near, far, device, experts):
    barrier = pltpu.get_barrier_semaphore()
    targets = [device((mine + r) % experts, block) for r in range(1, experts)]
    targets += [device(mine, near), device(mine, far)]
    for target in targets:
        pl.semaphore_signal(barrier, inc=1, device_id=target, device_id_type=MESH)
    pl.semaphore_wait(barrier, len(targets))


def over_far(r, every):
    return every > 0 and r % every == 0


def rounds(experts, groups):
    same = [r for r in range(experts) if r % groups == 0]
    return same + [r for r in range(experts) if r % groups]


DISPATCH_FAR = 4
COMBINE_FAR = 0
AHEAD = 4
LAG = 2


class Transfer:
    def __init__(self, src, dst, send, recv, slot, target):
        self.copies = [
            pltpu.make_async_remote_copy(
                src_ref=piece,
                dst_ref=landing,
                send_sem=send.at[slot + (k,)],
                recv_sem=recv.at[slot + (k,)],
                device_id=target,
                device_id_type=MESH,
            )
            for k, (piece, landing) in enumerate(zip(src, dst))
        ]

    def start(self):
        for copy in self.copies:
            copy.start()

    def wait_recv(self):
        for copy in self.copies:
            copy.wait_recv()

    def wait_send(self):
        for copy in self.copies:
            copy.wait_send()


def at(refs, *index):
    return [ref.at[index] for ref in refs]


def dispatch_kernel(experts, groups, pieces, *refs):
    bucket, out = refs[:pieces], refs[pieces : 2 * pieces]
    own_sem, a_send, a_recv, b_send, b_recv, c_send, c_recv = refs[2 * pieces :]
    mine, block, near, far, corner, device = place(groups)
    greet(mine, block, near, far, device, experts)

    order = rounds(experts, groups)
    spread, to_near, to_far, relay = {}, {}, {}, {}
    for r in reversed(order[1:]):
        peer = (mine + r) % experts
        spread[r] = Transfer(at(bucket, peer), at(out, block, mine), a_send, a_recv, (r,), device(peer, block))
        spread[r].start()
    own = [
        pltpu.make_async_copy(src, dst, own_sem.at[k])
        for k, (src, dst) in enumerate(zip(at(bucket, mine), at(out, block, mine)))
    ]
    for copy in own:
        copy.start()

    def forward(r):
        source = (mine + experts - r) % experts
        if over_far(r, DISPATCH_FAR):
            to_near[r].wait_recv()
            moved = at(out, near, source)
            relay[r] = Transfer(moved, moved, c_send, c_recv, (r,), device(mine, far))
        else:
            to_far[r].wait_recv()
            moved = at(out, far, source)
            relay[r] = Transfer(moved, moved, c_send, c_recv, (r,), device(mine, near))
        relay[r].start()

    for step, r in enumerate(order):
        source = (mine + experts - r) % experts
        dst = at(out, block, source)
        if r == 0:
            src = at(bucket, mine)
        else:
            spread[r].wait_recv()
            src = dst
        to_near[r] = Transfer(src, dst, b_send, b_recv, (0, r), device(mine, near))
        to_far[r] = Transfer(src, dst, b_send, b_recv, (1, r), device(mine, far))
        to_near[r].start()
        to_far[r].start()
        if step >= LAG:
            forward(order[step - LAG])
    for r in order[experts - LAG :]:
        forward(r)
    for r in order:
        if over_far(r, DISPATCH_FAR):
            to_far[r].wait_recv()
        else:
            to_near[r].wait_recv()
        relay[r].wait_recv()
    for r in order:
        if r:
            spread[r].wait_send()
        to_near[r].wait_send()
        to_far[r].wait_send()
        relay[r].wait_send()
    for copy in own:
        copy.wait()


def combine_kernel(experts, groups, pieces, *refs):
    part, ret, held, total, back = [refs[k * pieces : (k + 1) * pieces] for k in range(5)]
    a_send, a_recv, b_send, b_recv, c_send, c_recv = refs[5 * pieces :]
    mine, block, near, far, corner, device = place(groups)
    greet(mine, block, near, far, device, experts)

    def add(dst, *terms):
        for k in range(pieces):
            value = terms[0][k][...].astype(jnp.float32)
            for term in terms[1:]:
                value = value + term[k][...].astype(jnp.float32)
            dst[k][...] = value.astype(dst[k].dtype)

    order = rounds(experts, groups)[::-1]
    relay, to_near, to_far, home = {}, {}, {}, {}

    def open_round(r):
        source = (mine + experts - r) % experts
        target = far if over_far(r, COMBINE_FAR) else near
        relay[r] = Transfer(at(part, corner, source), at(held, 2, r), c_send, c_recv, (r,), device(mine, target))
        relay[r].start()
        if over_far(r, COMBINE_FAR):
            to_far[r] = Transfer(at(part, far, source), at(held, 1, r), b_send, b_recv, (1, r), device(mine, far))
            to_far[r].start()
        else:
            to_near[r] = Transfer(at(part, near, source), at(held, 0, r), b_send, b_recv, (0, r), device(mine, near))
            to_near[r].start()

    def send_home(r):
        source = (mine + experts - r) % experts
        to_near[r].wait_recv()
        to_far[r].wait_recv()
        terms = at(part, block, source), at(held, 0, r), at(held, 1, r)
        if r == 0:
            add(at(ret, mine), *terms)
        else:
            add(at(back, r), *terms)
            home[r] = Transfer(at(back, r), at(ret, mine), a_send, a_recv, (r,), device(source, block))
            home[r].start()

    for r in order[:AHEAD]:
        open_round(r)
    for step, r in enumerate(order):
        source = (mine + experts - r) % experts
        relay[r].wait_recv()
        if over_far(r, COMBINE_FAR):
            add(at(total, r), at(part, near, source), at(held, 2, r))
            to_near[r] = Transfer(at(total, r), at(held, 0, r), b_send, b_recv, (0, r), device(mine, near))
            to_near[r].start()
        else:
            add(at(total, r), at(part, far, source), at(held, 2, r))
            to_far[r] = Transfer(at(total, r), at(held, 1, r), b_send, b_recv, (1, r), device(mine, far))
            to_far[r].start()
        if step + AHEAD < experts:
            open_round(order[step + AHEAD])
        if step >= LAG:
            send_home(order[step - LAG])
    for r in order[experts - LAG :]:
        send_home(r)
    for r in order:
        if r:
            home[r].wait_recv()
            home[r].wait_send()
        relay[r].wait_send()
        to_near[r].wait_send()
        to_far[r].wait_send()


def sems(experts, pieces):
    dma = pltpu.SemaphoreType.DMA
    one, two = dma((experts, pieces)), dma((2, experts, pieces))
    return [one, one, two, two, one, one]


def dispatch(bucket, groups):
    experts, pieces = bucket[0].shape[0], len(bucket)
    return pl.pallas_call(
        functools.partial(dispatch_kernel, experts, groups, pieces),
        out_shape=[jax.ShapeDtypeStruct((SHARDS,) + piece.shape, piece.dtype) for piece in bucket],
        in_specs=[pl.BlockSpec(memory_space=pltpu.VMEM)] * pieces,
        out_specs=[pl.BlockSpec(memory_space=pl.ANY)] * pieces,
        scratch_shapes=[pltpu.SemaphoreType.DMA((pieces,))] + sems(experts, pieces),
        compiler_params=pltpu.CompilerParams(collective_id=0, has_side_effects=True),
        name="dispatch",
    )(*bucket)


def combine(part, groups):
    experts, pieces = part[0].shape[1], len(part)
    blocks = [(piece.shape[1:], piece.dtype) for piece in part]
    return pl.pallas_call(
        functools.partial(combine_kernel, experts, groups, pieces),
        out_shape=[jax.ShapeDtypeStruct(shape, kind) for shape, kind in blocks],
        in_specs=[pl.BlockSpec(memory_space=pltpu.VMEM)] * pieces,
        out_specs=[pl.BlockSpec(memory_space=pltpu.VMEM)] * pieces,
        scratch_shapes=[pltpu.VMEM((3,) + shape, kind) for shape, kind in blocks]
        + [pltpu.VMEM(shape, kind) for shape, kind in blocks] * 2
        + sems(experts, pieces),
        compiler_params=pltpu.CompilerParams(
            collective_id=1, has_side_effects=True, vmem_limit_bytes=60 * 2**20
        ),
        name="combine",
    )(*part)


def dot(left, right):
    return jnp.dot(left, right, preferred_element_type=jnp.float32)


def activate(gate_act, up_act):
    return (jax.nn.silu(gate_act) * up_act).astype(jnp.bfloat16)


def expert_block(rows, w_gate, w_up, w_down):
    hidden = activate(dot(rows, w_gate), dot(rows, w_up))
    return dot(hidden, w_down).astype(jnp.bfloat16)


def folded_block(rows, w_gate, w_up, w_down):
    half = rows.shape[1]

    def project(weight):
        left = dot(rows, weight[:half]).reshape(-1, 2, FOLD, weight.shape[1])
        right = dot(rows, weight[half:]).reshape(-1, 2, FOLD, weight.shape[1])
        return left[:, 0] + right[:, 1]

    hidden = activate(project(w_gate), project(w_up))
    twice = jnp.concatenate([hidden, hidden], axis=1).reshape(rows.shape[0], -1)
    upper = jnp.arange(rows.shape[0])[:, None] % (2 * FOLD) < FOLD
    return jnp.where(upper, dot(twice, w_down[:, :half]), dot(twice, w_down[:, half:])).astype(jnp.bfloat16)


def bucketed(tokens, routes, scores, gate_proj, up_proj, down_proj):
    node_count = lax.axis_size("node")
    local_count = lax.axis_size("local")
    token_count, model_width = tokens.shape
    top_count = routes.shape[1]
    groups = local_count // SHARDS
    experts = node_count * groups
    per_expert = max(
        2, token_count * top_count // experts + token_count * top_count // (4 * experts)
    )
    tile = 2 * FOLD
    half = model_width // 2
    full = per_expert // tile * tile
    folds = full > 0 and 0 < per_expert - full <= FOLD
    if not folds:
        full = (per_expert + tile - 1) // tile * tile
    cap = full + FOLD if folds else full
    weights = (SCALE * scores / jnp.sum(scores, axis=1, keepdims=True)).astype(jnp.bfloat16)
    labels = jnp.arange(experts, dtype=jnp.int32)
    matches = routes[:, :, None] == labels[None, None, :]
    routed = jnp.any(matches, axis=1)
    dense_weight = jnp.sum(jnp.where(matches, weights.astype(jnp.float32)[:, :, None], 0.0), axis=1)
    position = jnp.cumsum(routed.astype(jnp.int32), axis=0) - 1
    slot_ids = jnp.arange(cap, dtype=jnp.int32)
    pick = routed.T[:, None, :] & (position.T[:, None, :] == slot_ids[None, :, None])
    slot_pick = pick.astype(jnp.bfloat16)
    slot_weight = jnp.where(pick, dense_weight.T[:, None, :], 0.0).astype(jnp.bfloat16)

    def flat(slots):
        return slots.reshape(-1, slots.shape[-1])

    def halves(slots):
        none = jnp.zeros_like(slots)
        return flat(jnp.concatenate([slots, none], axis=1)), flat(jnp.concatenate([none, slots], axis=1))

    bucket = [dot(flat(slot_pick[:, :full]), tokens).astype(jnp.bfloat16).reshape(experts, full, model_width)]
    if folds:
        upper, lower = halves(slot_pick[:, full:])
        folded = (dot(upper, tokens[:, :half]) + dot(lower, tokens[:, half:])).astype(jnp.bfloat16)
        bucket.append(folded.reshape(experts, tile, half))
    gathered = dispatch(bucket, groups)
    blocks = expert_block, folded_block
    part = [
        blocks[k](flat(piece), gate_proj[0], up_proj[0], down_proj[0]).reshape(piece.shape)
        for k, piece in enumerate(gathered)
    ]
    returned = combine(part, groups)
    combined = dot(flat(slot_weight[:, :full]).T, flat(returned[0]))
    if folds:
        upper, lower = halves(slot_weight[:, full:])
        rows = flat(returned[1])
        combined = combined + jnp.concatenate([dot(upper.T, rows), dot(lower.T, rows)], axis=1)
    return combined.astype(jnp.bfloat16)


CORES = 2
SQUARES = 4
PARTS = 2
LATE = 2
DISPATCH_VIA_FAR = (5,)
COMBINE_VIA_FAR = (1, 3,)
SCHEDULE = [
    ("spread", 6), ("spread", 5), ("spread", 1), ("tables", 0), ("near", 0), ("near", 4),
    ("far", 0), ("near", 5), ("spread", 3), ("near", 1), ("near", 6), ("pass_on", 0),
    ("swap1", 5), ("far", 6), ("swap1", 4), ("spread", 2), ("far", 3), ("swap2", 6),
    ("near", 3), ("share", 0), ("pass_on", 6), ("spread", 7), ("compute", 0), ("pass_on", 3),
    ("far", 2), ("near", 2), ("far", 1), ("share", 3), ("swap0", 6), ("pass_on", 2),
    ("far", 7), ("compute", 3), ("swap3", 6), ("pass_on", 1), ("share", 2), ("near", 7),
    ("swap1", 6), ("far", 4), ("swap0", 4), ("pass_on", 7), ("far", 5), ("join", 0),
    ("swap0", 5), ("join", 3), ("share", 1), ("swap0", 7), ("swap2", 7), ("pass_on", 5),
    ("swap1", 7), ("side", 3), ("hop", 0), ("compute", 2), ("share", 7), ("pass_on", 4),
    ("swap3", 7), ("compute", 1), ("hop", 3), ("side", 0), ("swap3", 5), ("join", 2),
    ("share", 6), ("middle", 0), ("swap2", 4), ("compute", 7), ("hop", 2), ("swap2", 5),
    ("join", 1), ("swap3", 4), ("hop", 1), ("middle", 3), ("join", 7), ("share", 4),
    ("side", 1), ("side", 2), ("compute", 6), ("middle", 2), ("share", 5), ("finish", 3),
    ("join", 6), ("hop", 6), ("side", 6), ("compute", 4), ("hop", 7), ("middle", 6),
    ("finish", 2), ("join", 4), ("finish", 0), ("compute", 5), ("side", 7), ("middle", 7),
    ("join", 5), ("hop", 5), ("middle", 1), ("finish", 6), ("side", 5), ("hop", 4),
    ("middle", 5), ("finish", 7), ("side", 4), ("finish", 1), ("middle", 4), ("finish", 5),
    ("finish", 4),
]


class Flow:
    def __init__(self, **spec):
        self.spec = spec
        self.started = self.sent = self.landed = False

    def start(self):
        self.copy = pltpu.make_async_remote_copy(device_id_type=MESH, **self.spec)
        self.copy.start()
        self.started = True

    def wait_send(self):
        assert self.started
        if not self.sent:
            self.copy.wait_send()
        self.sent = True

    def wait_recv(self):
        assert self.started
        if not self.landed:
            self.copy.wait_recv()
        self.landed = True


def slots_of(token_count, top_count, experts):
    per_expert = max(2, token_count * top_count // experts + token_count * top_count // (4 * experts))
    seen = CORES * per_expert
    return seen, token_count - seen, 2 * seen - token_count


def flip(value, by):
    return 1 - value if by else value


def route(groups, private, shared, routes_ref, scores_ref, tokens_ref, lists_ref, pick_ref, weight_ref):
    node = lax.axis_index("node")
    local = lax.axis_index("local")
    side, core, half = node // CORES, node % CORES, local // SHARDS
    count = tokens_ref.shape[0]
    listed = count // 2
    swap = shared // 2
    names = routes_ref[...].astype(jnp.float32)
    first, second = names[0:1], names[1:2]
    score_first, score_second = scores_ref[0:1, :], scores_ref[1:2, :]
    total = score_first + score_second
    weight_first = (SCALE * score_first / total).astype(jnp.bfloat16).astype(jnp.float32)
    weight_second = (SCALE * score_second / total).astype(jnp.bfloat16).astype(jnp.float32)

    def named(expert):
        name = expert.astype(jnp.float32)
        return jnp.where(first == name, 1.0, 0.0) + jnp.where(second == name, 1.0, 0.0)

    def weight_row(expert):
        name = expert.astype(jnp.float32)
        return jnp.where(first == name, weight_first, 0.0) + jnp.where(second == name, weight_second, 0.0)

    def expert_at(dx, dh, dc):
        return (flip(side, dx) * CORES + flip(core, dc)) * groups + flip(half, dh)

    row = lax.broadcasted_iota(jnp.int32, (count, count), 0)
    col = lax.broadcasted_iota(jnp.int32, (count, count), 1)
    before = jnp.where(row < col, 1.0, 0.0).astype(jnp.bfloat16)
    slot = row.astype(jnp.float32)
    picks = []
    for dh in range(2):
        on = [jnp.minimum(named(expert_at(dx, dh, 0)) + named(expert_at(dx, dh, 1)), 1.0) for dx in range(2)]
        both = on[0] * on[1]
        only = [on[0] - both, on[1] - both]
        stack = jnp.concatenate([both, only[0], only[1], jnp.zeros((5, count), jnp.float32)], axis=0)
        rank = dot(stack.astype(jnp.bfloat16), before)
        both_rank = rank[0:1]
        both_count = jnp.sum(both, axis=1, keepdims=True)
        spilled = jnp.maximum(both_count - shared, 0.0)
        held = jnp.minimum(both_count, float(shared))

        def shared_slot(index):
            return jnp.where(index < swap, private + index, listed + private + index - swap)

        place = [spilled + rank[1:2], spilled + rank[2:3]]
        over = [shared_slot(held + place[0] - private), shared_slot(shared - 1 - (place[1] - private))]
        main = jnp.where(both_rank < shared, shared_slot(both_rank), both_rank - shared)
        main = jnp.where(both > 0, main, -1.0)
        for dx in range(2):
            here = jnp.where(place[dx] < private, dx * listed + place[dx], over[dx])
            main = jnp.where(only[dx] > 0, here, main)
        again = jnp.where((both > 0) & (both_rank >= shared), listed + both_rank - shared, -1.0)
        pick = jnp.where((slot == main) | (slot == again), 1.0, 0.0)
        picks.append(pick)
        for dx in range(2):
            mine = pick[dx * listed : (dx + 1) * listed]
            other = pick[(1 - dx) * listed + private : (2 - dx) * listed]
            r = 2 * dh + dx
            seen = jnp.concatenate(
                [mine, other, jnp.zeros((128 - listed - swap, count), jnp.float32)], axis=0
            ).astype(jnp.bfloat16)
            rows = jnp.concatenate(
                [weight_row(expert_at(dx, dh, dc)) for dc in range(2)] + [jnp.zeros((6, count), jnp.float32)], axis=0
            ).astype(jnp.bfloat16)
            values = lax.dot_general(rows, seen, (((1,), (1,)), ((), ())), preferred_element_type=jnp.float32)
            for dc in range(2):
                weight_ref[r, dc] = jnp.broadcast_to(values[dc : dc + 1], (8, 128))
    pick = jnp.concatenate(picks, axis=0).astype(jnp.bfloat16)
    for r in range(SQUARES):
        pick_ref[r] = pick[r * listed : (r + 1) * listed]
    width = 1024

    def fill(step, carry):
        columns = pl.ds(pl.multiple_of(step * width, width), width)
        rows = dot(pick, tokens_ref[:, columns]).astype(jnp.bfloat16)
        for r in range(SQUARES):
            lists_ref[r, :, columns] = rows[r * listed : (r + 1) * listed]
        return carry

    lax.fori_loop(0, tokens_ref.shape[1] // width, fill, 0)


def layer_kernel(
    groups, private, shared_slots, tokens, routes, scores, gate_hbm, up_hbm, down_hbm, combined,
    lists, pick, weight, ret, total, gate, up, down, rows_a, rows_b, table, given_a, given_b, extra, held_a, held_b, hidden,
    load_sem, own_sem, t_send, t_recv, send, recv,
):
    node = lax.axis_index("node")
    local = lax.axis_index("local")
    side, core = node // CORES, node % CORES
    half, block = local // SHARDS, local % SHARDS
    deep, across = block // 2, block % 2
    listed, swap = lists.shape[1], shared_slots // 2
    part = listed // PARTS
    rows, given, held = (rows_a, rows_b), (given_a, given_b), (held_a, held_b)
    lane = [rows[p].shape[2] for p in range(PARTS)]

    def device(r, dc, db):
        to_block = flip(deep, db // 2) * 2 + flip(across, db % 2)
        return (flip(side, r % 2) * CORES + flip(core, dc), flip(half, r // 2) * SHARDS + to_block)

    offsets = [(r, dc, db) for r in range(SQUARES) for dc in range(CORES) for db in range(SHARDS)][1:]
    barrier = pltpu.get_barrier_semaphore()
    for offset in offsets:
        pl.semaphore_signal(barrier, inc=1, device_id=device(*offset), device_id_type=MESH)

    loads = [
        pltpu.make_async_copy(src.at[0], dst, load_sem.at[k])
        for k, (src, dst) in enumerate(((gate_hbm, gate), (up_hbm, up), (down_hbm, down)))
    ]
    own = [
        pltpu.make_async_copy(
            lists.at[0, pl.ds(p * part, part)], rows[p].at[0, 0, pl.ds(0, part)], own_sem.at[p]
        )
        for p in range(PARTS)
    ]
    own.append(pltpu.make_async_copy(weight.at[0, 0], table.at[0, 0, 0], own_sem.at[PARTS]))
    for load in loads:
        load.start()
    route(groups, private, shared_slots, routes, scores, tokens, lists, pick, weight)
    pl.semaphore_wait(barrier, len(offsets))
    for copy in own:
        copy.start()
    waited = set()

    def once(*names):
        for name in names:
            if name not in waited:
                waited.add(name)
                (own + loads)[name].wait()

    everything = []

    def flow(kind, q, there, src, dst, target):
        made = Flow(
            src_ref=src, dst_ref=dst, send_sem=send.at[kind, q], recv_sem=recv.at[kind, there], device_id=target
        )
        everything.append(made)
        return made

    def piece(ref, r, p):
        return ref.at[r, pl.ds(p * part, part)]

    def entry(q, db):
        return rows[q // SQUARES].at[q % SQUARES, 0, pl.ds(db * part, part)]

    def last_rows(r, db):
        return rows[1].at[r, 0, pl.ds(db * part + part - swap, swap)]

    def other_rows(r, db):
        return rows[1].at[r, 0, pl.ds(SHARDS * part + db * swap, swap)]

    def other(q):
        return q + 1 - 2 * (q % 2)

    spread, near, far, relay, shared = {}, {}, {}, {}, {}
    out, hop, side_sum, far_sum, home, swapped, patch = {}, {}, {}, {}, {}, {}, {}
    y_way, z_way = device(0, 0, 1), device(0, 0, 2)
    for q in range(PARTS * SQUARES):
        p, r = q // SQUARES, q % SQUARES
        first = entry(q, 0) if r else piece(lists, 0, p)
        if r:
            spread[q] = flow(0, q, q, piece(lists, r, p), entry(q, 0), device(r, 0, 0))
            home[q] = flow(9, q, q, entry(q, 0), piece(ret, r, p), device(r, 0, 0))
        near[q] = flow(1, q, q, first, entry(q, 1), y_way)
        far[q] = flow(2, q, q, first, entry(q, 2), z_way)
        if q in DISPATCH_VIA_FAR:
            relay[q] = flow(3, q, q, entry(q, 1), entry(q, 3), z_way)
        else:
            relay[q] = flow(3, q, q, entry(q, 2), entry(q, 3), y_way)
        shared[q] = flow(4, q, q, rows[p].at[r, 0], rows[p].at[r, 1], device(0, 1, 0))
        out[q] = flow(5, q, q, rows[p].at[r, 1], given[p].at[r], device(0, 1, 0))
        early, late = (2, 1) if q in COMBINE_VIA_FAR else (1, 2)
        early_way, late_way = device(0, 0, early), device(0, 0, late)
        hop[q] = flow(6, q, q, entry(q, 3), held[p].at[2, r], early_way)
        side_sum[q] = flow(7, q, q, entry(q, early), held[p].at[0, r], early_way)
        far_sum[q] = flow(8, q, q, held[p].at[2, r], held[p].at[1, r], late_way)
        if p:
            for db in range(SHARDS):
                swapped[q, db] = flow(
                    10 + db, q, other(q), last_rows(r, db), other_rows(other(r), db), device(1, 0, 0)
                )
                patch[q, db] = flow(
                    14 + db,
                    q,
                    other(q),
                    other_rows(r, db),
                    extra.at[other(r), pl.ds(db * swap, swap)],
                    device(1, 0, 0),
                )
    tables = [
        Flow(
            src_ref=weight.at[r, dc],
            dst_ref=table.at[r, dc, db],
            send_sem=t_send.at[r, dc, db],
            recv_sem=t_recv.at[r, dc, db],
            device_id=device(r, dc, db),
        )
        for r, dc, db in offsets
    ]
    everything.extend(tables)

    def add_into(target, *terms):
        value = target[...].astype(jnp.float32)
        for term in terms:
            value = value + term[...].astype(jnp.float32)
        target[...] = value.astype(target.dtype)

    def landed(q, db):
        if db == 0:
            if q % SQUARES:
                spread[q].wait_recv()
            else:
                once(q // SQUARES)
        else:
            (None, near, far, relay)[db][q].wait_recv()

    def send_near(q):
        if q % SQUARES:
            spread[q].wait_recv()
        near[q].start()

    def send_far(q):
        if q % SQUARES:
            spread[q].wait_recv()
        far[q].start()

    def pass_on(q):
        landed(q, 1 if q in DISPATCH_VIA_FAR else 2)
        relay[q].start()

    def swap_rows(q, db):
        landed(q, db)
        swapped[q, db].start()

    def share(q):
        for db in range(SHARDS):
            landed(q, db)
        if q >= SQUARES:
            for db in range(SHARDS):
                swapped[other(q), db].wait_recv()
        shared[q].start()

    def column(q):
        p, r = q // SQUARES, q % SQUARES
        spans = [(part, p * part)] + ([(swap, listed)] if p else [])
        values = []
        for dc in range(CORES):
            for size, shift in spans:
                lanes = lax.broadcasted_iota(jnp.int32, (size, 128), 1)
                spots = lax.broadcasted_iota(jnp.int32, (size, 128), 0) + shift
                for db in range(SHARDS):
                    chosen = jnp.where(lanes == spots, table[r, dc, db, 0:1, :], 0.0)
                    values.append(jnp.sum(chosen, axis=1, keepdims=True))
        return jnp.concatenate(values, axis=0)

    def compute(q):
        p, r = q // SQUARES, q % SQUARES
        once(PARTS, PARTS + 1, PARTS + 2)
        for copy in tables:
            copy.wait_recv()
        shared[q].wait_recv()
        size = CORES * lane[p]
        scale = column(q)
        tile = 256

        def open_up(step, carry):
            columns = pl.ds(pl.multiple_of(step * tile, tile), tile)
            left = rows[p][r].reshape(size, down.shape[1])
            gate_act = dot(left, gate[:, columns])
            up_act = dot(left, up[:, columns])
            hidden[:size, columns] = (jax.nn.silu(gate_act) * up_act * scale).astype(jnp.bfloat16)
            return carry

        lax.fori_loop(0, gate.shape[1] // tile, open_up, 0)
        once(PARTS + 3)
        for sent in [near[q], far[q], relay[q], shared[q]] + [swapped[q, db] for db in range(SHARDS) if p]:
            sent.wait_send()
        wide = 1024

        def close(step, carry):
            columns = pl.ds(pl.multiple_of(step * wide, wide), wide)
            result = dot(hidden[:size], down[:, columns]).astype(jnp.bfloat16)
            rows[p][r, 0, :, columns] = result[: lane[p]]
            rows[p][r, 1, :, columns] = result[lane[p] :]
            return carry

        lax.fori_loop(0, down.shape[1] // wide, close, 0)
        out[q].start()

    def join(q):
        p, r = q // SQUARES, q % SQUARES
        out[q].wait_recv()
        if p:
            for db in (3, 1, 2, 0):
                add_into(other_rows(r, db), given[p].at[r, pl.ds(SHARDS * part + db * swap, swap)])
                patch[q, db].start()
        for db in range(SHARDS):
            add_into(entry(q, db), given[p].at[r, pl.ds(db * part, part)])

    def mended(q, db):
        if q >= SQUARES:
            patch[other(q), db].wait_recv()
            add_into(last_rows(q % SQUARES, db), extra.at[q % SQUARES, pl.ds(db * swap, swap)])

    def send_hop(q):
        mended(q, 3)
        hop[q].start()

    def send_side(q):
        mended(q, 2 if q in COMBINE_VIA_FAR else 1)
        side_sum[q].start()

    def middle(q):
        late = 1 if q in COMBINE_VIA_FAR else 2
        mended(q, late)
        hop[q].wait_recv()
        add_into(held[q // SQUARES].at[2, q % SQUARES], entry(q, late))
        far_sum[q].start()

    def finish(q):
        p, r = q // SQUARES, q % SQUARES
        mended(q, 0)
        side_sum[q].wait_recv()
        far_sum[q].wait_recv()
        if r:
            add_into(entry(q, 0), held[p].at[0, r], held[p].at[1, r])
            home[q].start()
        else:
            value = entry(q, 0)[...].astype(jnp.float32)
            value = value + held[p][0, r].astype(jnp.float32) + held[p][1, r].astype(jnp.float32)
            piece(ret, 0, p)[...] = value.astype(ret.dtype)

    def add_up(chunks, ending):
        for q in chunks:
            if q % SQUARES:
                home[q].wait_recv()
        wide = 1024
        picked = jnp.concatenate([piece(pick, q % SQUARES, q // SQUARES)[...] for q in chunks], axis=0)

        def step(k, carry):
            columns = pl.ds(pl.multiple_of(k * wide, wide), wide)
            back = jnp.concatenate(
                [ret[q % SQUARES, pl.ds(q // SQUARES * part, part), columns] for q in chunks], axis=0
            )
            value = lax.dot_general(picked, back, (((0,), (0,)), ((), ())), preferred_element_type=jnp.float32)
            if ending:
                combined[:, columns] = (total[:, columns] + value).astype(combined.dtype)
            else:
                total[:, columns] = value
            return carry

        lax.fori_loop(0, ret.shape[2] // wide, step, 0)

    steps = dict(
        spread=lambda q: spread[q].start(), near=send_near, far=send_far, pass_on=pass_on, share=share,
        compute=compute, join=join, hop=send_hop, side=send_side, middle=middle, finish=finish,
        tables=lambda q: [copy.start() for copy in tables],
    )
    for db in range(SHARDS):
        steps[f"swap{db}"] = functools.partial(swap_rows, db=db)
    for name, q in SCHEDULE:
        steps[name](q)
    last = [q for name, q in SCHEDULE if name == "finish"]
    add_up(last[:-LATE], False)
    add_up(last[-LATE:], True)
    once(*range(PARTS + 4))
    for made in everything:
        made.wait_recv()
        made.wait_send()


def layer(tokens, routes, scores, gate_proj, up_proj, down_proj, groups, private, shared):
    count, model_width = tokens.shape
    listed, swap = count // 2, shared // 2
    hidden_width = gate_proj.shape[2]
    part = listed // PARTS
    lanes = (SHARDS * part, SHARDS * (part + swap))
    dma = pltpu.SemaphoreType.DMA
    vmem = pl.BlockSpec(memory_space=pltpu.VMEM)
    hbm = pl.BlockSpec(memory_space=pl.ANY)

    def space(*shape):
        return pltpu.VMEM(shape, jnp.bfloat16)

    return pl.pallas_call(
        functools.partial(layer_kernel, groups, private, shared),
        out_shape=jax.ShapeDtypeStruct(tokens.shape, tokens.dtype),
        in_specs=[vmem, vmem, vmem, hbm, hbm, hbm],
        out_specs=vmem,
        scratch_shapes=[
            space(SQUARES, listed, model_width),
            space(SQUARES, listed, count),
            pltpu.VMEM((SQUARES, CORES, 8, 128), jnp.float32),
            space(SQUARES, listed, model_width),
            pltpu.VMEM((count, model_width), jnp.float32),
            space(*gate_proj.shape[1:]),
            space(*up_proj.shape[1:]),
            space(*down_proj.shape[1:]),
            space(SQUARES, CORES, lanes[0], model_width),
            space(SQUARES, CORES, lanes[1], model_width),
            pltpu.VMEM((SQUARES, CORES, SHARDS, 8, 128), jnp.float32),
            space(SQUARES, lanes[0], model_width),
            space(SQUARES, lanes[1], model_width),
            space(SQUARES, SHARDS * swap, model_width),
            space(3, SQUARES, part, model_width),
            space(3, SQUARES, part, model_width),
            space(CORES * lanes[1], hidden_width),
            dma((3,)),
            dma((PARTS + 1,)),
            dma((SQUARES, CORES, SHARDS)),
            dma((SQUARES, CORES, SHARDS)),
            dma((18, PARTS * SQUARES)),
            dma((18, PARTS * SQUARES)),
        ],
        compiler_params=pltpu.CompilerParams(
            collective_id=2, has_side_effects=True, vmem_limit_bytes=67043328
        ),
        name="layer",
    )(tokens, routes, scores, gate_proj, up_proj, down_proj)


def per_device(tokens, routes, scores, gate_proj, up_proj, down_proj):
    node_count = lax.axis_size("node")
    local_count = lax.axis_size("local")
    token_count, top_count = routes.shape
    groups = local_count // SHARDS
    experts = node_count * groups
    seen, private, shared = slots_of(token_count, top_count, experts)
    square = node_count == 2 * CORES and groups == 2 and top_count == 2
    fits = private > 0 and shared > 0 and private % 8 == 0 and shared % 16 == 0 and token_count % 32 == 0
    if not (square and fits):
        return bucketed(tokens, routes, scores, gate_proj, up_proj, down_proj)
    return layer(tokens, routes.T, scores.T, gate_proj, up_proj, down_proj, groups, private, shared)


def solution(mesh):
    return jax.shard_map(
        per_device,
        mesh=mesh,
        in_specs=(
            P(("node", "local"), None),
            P(("node", "local"), None),
            P(("node", "local"), None),
            P(("node", "local"), None, None),
            P(("node", "local"), None, None),
            P(("node", "local"), None, None),
        ),
        out_specs=P(("node", "local"), None),
        check_vma=False,
    )
```
